768 devices in a mesh: row: 96 (over z, y), col: 8 (over x, core).
Axes of the slice: x: 4, y: 8, z: 12, core: 2. Of those that a mesh axis runs over, the one named last changes fastest.
Arguments:
- concentration: float32 [96, 96, 768], P('row', 'col'), may hold values from -2.5 to 2.5
- plane_counts: int32 [8], replicated, may hold values from 1 to 73, 385 in all
Outputs:
- new_concentration: float32 [96, 96, 768], P('row', 'col')
- chemical_potential: float32 [96, 96, 768], P('row', 'col')
- plane_power: float32 [584], P('col')
The draws below stay inside these ranges and needn't reach their ends.
Inputs may be any that keep to these rules, and one draw needn't show every extreme that they name: Column device j owns the x wavenumber planes o_j to o_j + plane_counts[j] - 1, with o_j the sum of the counts before it; the counts sum to 385 and the largest is exactly 73.
All inputs are finite; a program needn't handle non-finite values.
Results may differ from the reference program's by a relative error of at most 0.000096.
Values sent between devices are 32-bit elements; how exact they have to be, the bound alone decides.
A program may use at most 32 MiB of HBM per device.

```python
import math
import jax
import jax.numpy as jnp
import numpy as np

NX = 768
NKX = 385
NY = 96
NZ = 96
KX_MOST = 73
N_COL = 8


def shard_levels(stream_key, shape, pieces, low, high):
    factor_of, own = 1.0, jax.random.fold_in(stream_key, 6)
    for dim, shards_of in pieces:
        steps = jnp.exp(jax.random.uniform(jax.random.fold_in(own, dim), (shards_of,), jnp.float32, low / len(pieces), high / len(pieces)))
        factor_of = factor_of * jnp.repeat(steps, shape[dim] // shards_of).reshape([-1 if axis == dim else 1 for axis in range(len(shape))])
    return factor_of


def split_up(number_of, total, reach, skew):
    portions = [(1 << 20) // math.isqrt(rank ** skew) + 1 for rank in range(2, number_of + 1)]
    rest, holding = total - reach - (number_of - 1), [1] * (number_of - 1)
    while rest > 0:
        free = [i for i in range(number_of - 1) if holding[i] < reach]
        whole, remaining = sum([portions[i] for i in free]), rest
        for i in free:
            extra = min(reach - holding[i], max(1, remaining * portions[i] // whole), rest)
            holding[i] = holding[i] + extra
            rest = rest - extra
    return np.array([reach] + holding)


def ragged(rng, count, total, bound, skew):
    if count == 2:
        one = jax.random.randint(rng, (), max(1, total - bound), min(bound, total - 1) + 1)
        return jnp.stack([one, total - one])
    tallies = jnp.asarray(split_up(count, total, bound, skew), jnp.int32)
    twos = (count - 1) // 2
    giver, taker = tallies[1:1 + 2 * twos:2], tallies[2:2 + 2 * twos:2]
    slack = jnp.minimum(giver - 1, bound - taker)
    shifted = jax.random.randint(jax.random.fold_in(rng, 1), (twos,), 0, 1 << 20) % (slack + 1)
    tallies = tallies.at[1:1 + 2 * twos:2].set(giver - shifted).at[2:2 + 2 * twos:2].set(taker + shifted)
    return tallies[jax.random.permutation(jax.random.fold_in(rng, 2), count)]


def bell_draw(rng, dims, width, reach, shards=(), held_as=jnp.bfloat16):
    level = shard_levels(rng, dims, shards, -0.22, 0.18) if shards else 1.0
    array = jax.random.normal(rng, dims, jnp.float32) * width * level
    return jnp.minimum(jnp.maximum(array, -reach), reach).astype(held_as)


def setup_inputs(seed: int = 0) -> dict:
    seeds = jax.random.split(jax.random.key(seed), 3)
    return {
        "concentration": bell_draw(seeds[0], (NZ, NY, NX), 0.5, 2.5, ((0, 96), (1, 8)), jnp.float32),
        "plane_counts": ragged(seeds[1], N_COL, NKX, KX_MOST, 2).astype(jnp.int32),
    }


time_step = 16.0
grad_coeff = 1.0
power_floor = 1e-6


def magnitude(points):
    positions = jnp.arange(points, dtype=jnp.int32)
    folded = jnp.minimum(positions, points - positions).astype(jnp.float32)
    return folded * (2.0 * math.pi / points)


def reference(concentration, plane_counts):
    nonlinear = concentration * concentration * concentration - concentration
    conc_hat = jnp.fft.rfftn(concentration, axes=(0, 1, 2))
    chem_hat = jnp.fft.rfftn(nonlinear, axes=(0, 1, 2))
    x_waves = jnp.arange(NKX, dtype=jnp.float32) * (2.0 * math.pi / NX)
    z_waves = magnitude(NZ)
    y_waves = magnitude(NY)
    squared = z_waves[:, None, None] ** 2 + y_waves[None, :, None] ** 2 + x_waves[None, None, :] ** 2
    damping = 1.0 + time_step * grad_coeff * squared * squared
    new_hat = (conc_hat - time_step * squared * chem_hat) / damping
    potential_hat = chem_hat + grad_coeff * squared * new_hat
    new_concentration = jnp.fft.irfftn(new_hat, s=(NZ, NY, NX), axes=(0, 1, 2)).astype(jnp.float32)
    chemical_potential = jnp.fft.irfftn(potential_hat, s=(NZ, NY, NX), axes=(0, 1, 2)).astype(jnp.float32)
    divisor = float(NX * NY * NY * NZ * NZ)
    power = jnp.sum(jnp.real(new_hat) ** 2 + jnp.imag(new_hat) ** 2, axis=(0, 1)) / divisor
    log_power = jnp.log(power + power_floor).astype(jnp.float32)
    counts = plane_counts.astype(jnp.int32)
    starts = jnp.cumsum(counts) - counts
    slot_ids = jnp.arange(KX_MOST, dtype=jnp.int32)
    plane_ids = jnp.clip(starts[:, None] + slot_ids[None, :], 0, NKX - 1).astype(jnp.int32)
    picked = jnp.take(log_power, plane_ids)
    in_use = slot_ids[None, :] < counts[:, None]
    plane_power = jnp.where(in_use, picked, jnp.zeros_like(picked)).reshape(-1).astype(jnp.float32)
    return new_concentration, chemical_potential, plane_power
```

```python
import functools
import math

import jax
import jax.numpy as jnp
import numpy as np
from jax import lax
from jax.experimental import pallas as pl
from jax.experimental.pallas import tpu as pltpu
from jax.sharding import PartitionSpec as P

MESH = pl.DeviceIdType.MESH
NX, NY, NZ = 768, 96, 96
HALF = NX // 2
COLS, ROWS = 8, 96
YB = NY // COLS
LANES = 128
SLOTS = 64
EVEN, ODD = 49, 48
SPARE = 15
PLANES = NX // 2 + 1
KX_MOST = 73
BLOCK = 2 * YB
WIDE = 2 * NY

time_step = 16.0
grad_coeff = 1.0
power_floor = 1e-6


def split(table):
    high = table.astype(np.float32).astype(jnp.bfloat16)
    low = (table - high.astype(np.float64)).astype(np.float32).astype(jnp.bfloat16)
    return np.stack([high, low])


def plane_of(col, slot):
    even = 2 * (EVEN * col + slot)
    odd = 2 * (ODD * (col - COLS // 2) + slot) + 1
    in_even = (slot < EVEN) & (even < PLANES)
    in_odd = slot < ODD
    low_col = col < COLS // 2
    return np.where(low_col, np.where(in_even, even, -1), np.where(in_odd, odd, -1))


@functools.cache
def tables():
    col = np.arange(COLS)[:, None]
    slot = np.arange(SLOTS)[None, :]
    plane = plane_of(col, slot)
    used = plane >= 0
    cells = np.arange(HALF)[:, None, None]
    phase = 2.0 * math.pi / NX * ((cells * np.maximum(plane, 0)[None]) % NX)
    x_table = np.stack([np.cos(phase) * used, -np.sin(phase) * used], axis=2)
    x_table = x_table.reshape(HALF, 2, COLS // 2 * LANES).transpose(1, 0, 2)
    edge = (plane == 0) | (2 * plane == NX)
    weight = np.where(used, np.where(edge, 1.0, 2.0), 0.0) / float(NX * NY * NZ)
    weight = np.concatenate([weight, weight], axis=1).reshape(COLS, 1, LANES)

    index = np.arange(96)
    phase = 2.0 * math.pi / 96 * ((index[:, None] * index[None, :]) % 96)
    cosine, sine = np.cos(phase), np.sin(phase)
    full = np.stack([np.stack([cosine, sine], 1), np.stack([-sine, cosine], 1)])
    full = full.reshape(2, 96, 2, 96)
    by_block = full.reshape(2, 96, 2, COLS, YB)
    y_forward = by_block.transpose(1, 0, 3, 2, 4).reshape(WIDE, WIDE)
    z_forward = full.transpose(0, 1, 3, 2).reshape(WIDE, WIDE)
    square = np.stack([split(y_forward), split(z_forward), split(z_forward.T), split(y_forward.T)])

    lane = np.arange(LANES)[None, None, :]
    part = np.arange(2)[None, :, None]
    inside = lane % SLOTS
    packed = SPARE * (2 * part + lane // SLOTS) + inside - EVEN
    ids = plane_of(np.arange(COLS)[:, None, None], packed)
    ids = np.where((inside >= EVEN) & (packed < EVEN), ids, -1).astype(np.int32).reshape(2 * COLS, LANES)
    return (
        np.stack([split(x_table[0]), split(x_table[1])]),
        square,
        weight.astype(np.float32),
        ids,
    )


def halves(value):
    high = value.astype(jnp.bfloat16)
    low = (value - high.astype(jnp.float32)).astype(jnp.bfloat16)
    return high, low


def product(a, b, contract):
    return lax.dot_general(a, b, (contract, ((), ())), preferred_element_type=jnp.float32)


def table_times(table, value):
    high, low = halves(value)
    inner = ((1,), (0,))
    return product(table[0], high, inner) + (product(table[1], high, inner) + product(table[0], low, inner))


def times_table(value, table, contract):
    high, low = halves(value)
    return product(high, table[0], contract) + (product(low, table[0], contract) + product(high, table[1], contract))


def signal(semaphore, row, col):
    pl.semaphore_signal(semaphore, inc=1, device_id=(row, col), device_id_type=MESH)


def col_exchange(source, target, send, receive, row, col):
    mine = pl.ds(pl.multiple_of(col * BLOCK, 8), BLOCK)
    for step in range(1, COLS):
        peer = lax.rem(col + step, COLS)
        theirs = pl.ds(pl.multiple_of(peer * BLOCK, 8), BLOCK)
        pltpu.make_async_remote_copy(
            source.at[theirs], target.at[mine], send, receive, device_id=(row, peer), device_id_type=MESH
        ).start()
    pltpu.make_async_copy(source.at[mine], target.at[mine], receive).start()


def row_exchange(source, target, send, receive, row, col):
    mine = pl.ds(2 * row, 2)

    def one(step, carry):
        peer = lax.rem(row + step, ROWS)
        pltpu.make_async_remote_copy(
            source.at[pl.ds(2 * peer, 2)], target.at[mine], send, receive, device_id=(peer, col), device_id_type=MESH
        ).start()
        return carry

    lax.fori_loop(1, ROWS, one, 0)
    pltpu.make_async_copy(source.at[mine], target.at[mine], receive).start()


def arrived(buffer, semaphore):
    pltpu.make_async_copy(buffer, buffer, semaphore).wait()


def kernel(
    counts, cells, x_hbm, square_hbm, weight, ids, conc_out, chem_out, power_out,
    x_table, square, buffers, table_sems, send_sems, recv_sems,
):
    row, col = lax.axis_index("row"), lax.axis_index("col")
    barrier = pltpu.get_barrier_semaphore()

    def greet(step, carry):
        signal(barrier, lax.rem(row + step, ROWS), col)
        return carry

    for step in range(1, COLS):
        signal(barrier, row, lax.rem(col + step, COLS))
    lax.fori_loop(1, ROWS, greet, 0)
    loads = [
        pltpu.make_async_copy(x_hbm.at[0], x_table.at[0], table_sems.at[0]),
        pltpu.make_async_copy(x_hbm.at[1], x_table.at[1], table_sems.at[1]),
        pltpu.make_async_copy(square_hbm, square, table_sems.at[2]),
    ]
    for load in loads:
        load.start()

    lane = lax.broadcasted_iota(jnp.int32, (16, LANES), 1)
    first = lane < SLOTS
    conc = jnp.concatenate([cells[:, 0, :], jnp.zeros((16 - YB, NX), jnp.float32)])
    chem = conc * conc * conc - conc
    both = jnp.concatenate([conc, chem])
    folded = (both[:, :HALF] + both[:, HALF:], both[:, :HALF] - both[:, HALF:])
    out = buffers.at[0]
    for parity in range(2):
        loads[parity].wait()
        spectrum = times_table(folded[parity], x_table.at[parity], ((1,), (0,)))
        for j in range(COLS // 2):
            part = spectrum[:, j * LANES:(j + 1) * LANES]
            top, bottom = part[:16], part[16:]
            base = (parity * (COLS // 2) + j) * BLOCK
            real = jnp.where(first, top, pltpu.roll(bottom, SLOTS, 1))
            imag = jnp.where(first, pltpu.roll(top, SLOTS, 1), bottom)
            out[base:base + YB, :] = real[:YB]
            out[base + YB:base + BLOCK, :] = imag[:YB]

    pl.semaphore_wait(barrier, COLS - 1 + ROWS - 1)
    col_exchange(buffers.at[0], buffers.at[1], send_sems.at[0], recv_sems.at[0], row, col)
    loads[2].wait()

    lane_w = lax.broadcasted_iota(jnp.int32, (NZ, LANES), 1)
    kz = lax.broadcasted_iota(jnp.int32, (NZ, LANES), 0)
    slot = lax.rem(lane_w, SLOTS)
    low_col = col < COLS // 2
    kx = 2 * slot + jnp.where(low_col, 2 * EVEN * col, 2 * ODD * (col - COLS // 2) + 1)
    x_wave = kx.astype(jnp.float32) * (2.0 * math.pi / NX)
    y_wave = jnp.minimum(row, NY - row).astype(jnp.float32) * (2.0 * math.pi / NY)
    z_wave = jnp.minimum(kz, NZ - kz).astype(jnp.float32) * (2.0 * math.pi / NZ)
    squared = z_wave * z_wave + y_wave * y_wave + x_wave * x_wave
    damping = 1.0 / (1.0 + time_step * grad_coeff * squared * squared)
    mixing = jnp.where(lane_w < SLOTS, -time_step * squared, grad_coeff * squared)

    arrived(buffers.at[1], recv_sems.at[0])
    buffers[2] = table_times(square.at[0], buffers[1])
    row_exchange(buffers.at[2], buffers.at[3], send_sems.at[1], recv_sems.at[1], row, col)
    arrived(buffers.at[3], recv_sems.at[1])
    hat = table_times(square.at[1], buffers[3])
    real, imag = hat[:NZ], hat[NZ:]
    real = (real + mixing * pltpu.roll(real, SLOTS, 1)) * damping
    imag = (imag + mixing * pltpu.roll(imag, SLOTS, 1)) * damping
    partial = jnp.sum(real * real + imag * imag, axis=0, keepdims=True)
    partial = jnp.broadcast_to(partial, (8, LANES))
    lane_8 = lax.broadcasted_iota(jnp.int32, (8, LANES), 1)
    sub_8 = lax.broadcasted_iota(jnp.int32, (8, LANES), 0)
    spare_8 = lax.rem(lane_8, SLOTS) >= EVEN
    chunks = [
        pltpu.roll(partial, (EVEN + SLOTS * (k % 2) - SPARE * k) % LANES, 1) for k in range(4)
    ]
    packed = jnp.where(
        lax.rem(sub_8, 2) == 0,
        jnp.where(lane_8 < SLOTS, chunks[0], chunks[1]),
        jnp.where(lane_8 < SLOTS, chunks[2], chunks[3]),
    )
    field = table_times(square.at[2], jnp.concatenate([real, imag])).reshape(WIDE // 8, 8, LANES)
    buffers[4] = jnp.where(spare_8[None], packed[None], field).reshape(WIDE, LANES)
    row_exchange(buffers.at[4], buffers.at[5], send_sems.at[2], recv_sems.at[2], row, col)
    arrived(buffers.at[5], recv_sems.at[2])
    gathered = buffers[5]
    total = jnp.sum(gathered.reshape(WIDE // 8, 8, LANES), axis=0)
    total = total + pltpu.roll(total, 2, 0)
    total = total + pltpu.roll(total, 4, 0)
    even_total = jnp.broadcast_to(total[0:1], (BLOCK, LANES))
    odd_total = jnp.broadcast_to(total[1:2], (BLOCK, LANES))
    sub_b = lax.broadcasted_iota(jnp.int32, (BLOCK, LANES), 0)
    lane_b = lax.broadcasted_iota(jnp.int32, (BLOCK, LANES), 1)
    totals = jnp.where(sub_b < YB, even_total, odd_total)
    spare_b = lax.rem(lane_b, SLOTS) >= EVEN
    field = table_times(square.at[3], gathered).reshape(COLS, BLOCK, LANES)
    buffers[6] = jnp.where(spare_b[None], totals[None], field).reshape(WIDE, LANES)
    col_exchange(buffers.at[6], buffers.at[7], send_sems.at[3], recv_sems.at[3], row, col)

    start = jnp.int32(0)
    for i in range(COLS):
        start = start + jnp.where(i < col, counts[i], 0)
    mine = counts[col]
    wanted = lax.broadcasted_iota(jnp.int32, (80, LANES), 0) + start

    arrived(buffers.at[7], recv_sems.at[3])
    last = buffers.at[7]
    sums = []
    for parity in range(2):
        pieces = []
        for j in range(COLS // 2):
            c = parity * (COLS // 2) + j
            pad = jnp.zeros((16 - YB, LANES), jnp.float32)
            real = jnp.concatenate([last[c * BLOCK:c * BLOCK + YB, :], pad])
            imag = jnp.concatenate([last[c * BLOCK + YB:(c + 1) * BLOCK, :], pad])
            scale = weight[c]
            keep = scale > 0.0
            top = jnp.where(first, real, pltpu.roll(imag, SLOTS, 1))
            bottom = jnp.where(first, pltpu.roll(real, SLOTS, 1), imag)
            pieces.append(jnp.where(keep, jnp.concatenate([top, bottom]) * scale, 0.0))
        sums.append(times_table(jnp.concatenate(pieces, axis=1), x_table.at[parity], ((1,), (1,))))
    front, back = sums[0] + sums[1], sums[0] - sums[1]
    conc_out[:, 0, :HALF] = front[:YB]
    conc_out[:, 0, HALF:] = back[:YB]
    chem_out[:, 0, :HALF] = front[16:16 + YB]
    chem_out[:, 0, HALF:] = back[16:16 + YB]

    found = jnp.zeros((80, LANES), jnp.float32)
    for c in range(COLS):
        for part in range(2):
            at = c * BLOCK + part * YB
            values = jnp.broadcast_to(last[at:at + 1, :], (80, LANES))
            found = found + jnp.where(ids[2 * c + part:2 * c + part + 1, :] == wanted, values, 0.0)
    power = lax.dot_general(
        jnp.ones((8, LANES), jnp.float32), found, (((1,), (1,)), ((), ())),
        precision=lax.Precision.HIGHEST, preferred_element_type=jnp.float32,
    )
    power = jnp.log(power * (1.0 / float(NX * NY * NY * NZ * NZ)) + power_floor)
    power = jnp.where(lax.broadcasted_iota(jnp.int32, (8, 80), 1) < mine, power, 0.0)
    power_out[...] = power[0:1, :KX_MOST]

    for i, (buffer, left) in enumerate(((0, BLOCK), (2, 2), (4, 2), (6, BLOCK))):
        sent = buffers.at[buffer, pl.ds(0, WIDE - left)]
        arrived(sent, send_sems.at[i])


def shards(concentration, plane_counts):
    x_table, square, weight, ids = (jnp.asarray(t) for t in tables())
    vmem = pl.BlockSpec(memory_space=pltpu.VMEM)
    anywhere = pl.BlockSpec(memory_space=pl.ANY)
    smem = pl.BlockSpec(memory_space=pltpu.SMEM)
    conc, chem, power = pl.pallas_call(
        kernel,
        out_shape=(
            jax.ShapeDtypeStruct((YB, 1, NX), jnp.float32),
            jax.ShapeDtypeStruct((YB, 1, NX), jnp.float32),
            jax.ShapeDtypeStruct((1, KX_MOST), jnp.float32),
        ),
        in_specs=[smem, vmem, anywhere, anywhere, vmem, vmem],
        out_specs=(vmem, vmem, vmem),
        scratch_shapes=[
            pltpu.VMEM(x_table.shape, jnp.bfloat16),
            pltpu.VMEM(square.shape, jnp.bfloat16),
            pltpu.VMEM((8, WIDE, LANES), jnp.float32),
            pltpu.SemaphoreType.DMA((3,)),
            pltpu.SemaphoreType.DMA((4,)),
            pltpu.SemaphoreType.DMA((4,)),
        ],
        compiler_params=pltpu.CompilerParams(collective_id=0, has_side_effects=True),
    )(plane_counts, concentration.reshape(YB, 1, NX), x_table, square, weight, ids)
    return conc.reshape(1, YB, NX), chem.reshape(1, YB, NX), power.reshape(KX_MOST)


def solution(mesh):
    return jax.shard_map(
        shards,
        mesh=mesh,
        in_specs=(P("row", "col", None), P()),
        out_specs=(P("row", "col", None), P("row", "col", None), P("col")),
        check_vma=False,
    )
```

```python
import functools
import math

import jax
import jax.numpy as jnp
import numpy as np
from jax import lax
from jax.experimental import pallas as pl
from jax.experimental.pallas import tpu as pltpu
from jax.sharding import PartitionSpec as P

MESH = pl.DeviceIdType.MESH
NX, NY, NZ = 768, 96, 96
HALF = NX // 2
COLS, ROWS = 8, 96
RING_Z, RING_Y = 12, 8
FAR_Y = (4, 3, 5, 2, 6, 1, 7)
NEAR_Z = (1, 2, 3, -1, -2, -3)
NEAR_Y = (1, 2, -1, -2)
YB = NY // COLS
LANES = 128
SLOTS = 64
EVEN, ODD = 49, 48
SPARE = 15
PLANES = NX // 2 + 1
KX_MOST = 73
BLOCK = 2 * YB
WIDE = 2 * NY
X_SHARE = COLS // 2 * LANES
VMEM = 67_043_328
ROOM = 10_600_000

time_step = 16.0
grad_coeff = 1.0
power_floor = 1e-6


def split(table):
    high = table.astype(np.float32).astype(jnp.bfloat16)
    low = (table - high.astype(np.float64)).astype(np.float32).astype(jnp.bfloat16)
    return np.stack([high, low])


def plane_of(col, slot, np=np):
    even = 2 * (EVEN * col + slot)
    odd = 2 * (ODD * (col - COLS // 2) + slot) + 1
    in_even = (slot < EVEN) & (even < PLANES)
    in_odd = slot < ODD
    low_col = col < COLS // 2
    return np.where(low_col, np.where(in_even, even, -1), np.where(in_odd, odd, -1))


@functools.cache
def tables():
    col = np.arange(COLS)[:, None]
    slot = np.arange(SLOTS)[None, :]
    plane = plane_of(col, slot)
    used = plane >= 0
    cells = np.arange(HALF)[:, None, None]
    phase = 2.0 * math.pi / NX * ((cells * np.maximum(plane, 0)[None]) % NX)
    x_table = np.stack([np.cos(phase) * used, -np.sin(phase) * used], axis=2)
    x_table = x_table.reshape(HALF, 2, COLS // 2 * LANES).transpose(1, 0, 2)

    index = np.arange(96)
    phase = 2.0 * math.pi / 96 * ((index[:, None] * index[None, :]) % 96)
    cosine, sine = np.cos(phase), np.sin(phase)
    full = np.stack([np.stack([cosine, sine], 1), np.stack([-sine, cosine], 1)])
    full = full.reshape(2, 96, 2, 96)
    by_block = full.reshape(2, 96, 2, COLS, YB)
    y_forward = by_block.transpose(1, 0, 3, 2, 4).reshape(WIDE, WIDE)
    z_forward = full.transpose(0, 1, 3, 2).reshape(WIDE, WIDE)
    square = np.zeros((2, HALF, X_SHARE), jnp.bfloat16)
    for k, table in enumerate((y_forward, z_forward, z_forward.T, y_forward.T)):
        square[:, k // 2 * WIDE:(k // 2 + 1) * WIDE, k % 2 * 256:k % 2 * 256 + WIDE] = split(table)
    return np.concatenate([split(x_table[0]), split(x_table[1]), square])


def halves(value):
    high = value.astype(jnp.bfloat16)
    low = (value - high.astype(jnp.float32)).astype(jnp.bfloat16)
    return high, low


def product(a, b, contract):
    return lax.dot_general(a, b, (contract, ((), ())), preferred_element_type=jnp.float32)


def table_times(table, value):
    high, low = halves(value)
    inner = ((1,), (0,))
    return product(table[0], high, inner) + (product(table[1], high, inner) + product(table[0], low, inner))


def times_table(value, table, contract):
    high, low = halves(value)
    return product(high, table[0], contract) + (product(low, table[0], contract) + product(high, table[1], contract))


def signal(semaphore, row, col):
    pl.semaphore_signal(semaphore, inc=1, device_id=(row, col), device_id_type=MESH)


def col_exchange(source, target, send, receive, row, col):
    mine = pl.ds(pl.multiple_of(col * BLOCK, 8), BLOCK)
    for step in range(1, COLS):
        peer = lax.rem(col + step, COLS)
        theirs = pl.ds(pl.multiple_of(peer * BLOCK, 8), BLOCK)
        pltpu.make_async_remote_copy(
            source.at[theirs], target.at[mine], send, receive, device_id=(row, peer), device_id_type=MESH
        ).start()
    pltpu.make_async_copy(source.at[mine], target.at[mine], receive).start()


def row_exchange(source, target, send, receive, row, col):
    mine = pl.ds(2 * row, 2)
    row_z, row_y = row // RING_Y, lax.rem(row, RING_Y)

    def one(step_z, step_y):
        peer = lax.rem(row_z + step_z, RING_Z) * RING_Y + lax.rem(row_y + step_y, RING_Y)
        pltpu.make_async_remote_copy(
            source.at[pl.ds(2 * peer, 2)], target.at[mine], send, receive, device_id=(peer, col), device_id_type=MESH
        ).start()

    def plane(i, carry):
        step_z = RING_Z // 2 + (1 - 2 * lax.rem(i, 2)) * ((i + 1) // 2)
        for step_y in FAR_Y + (0,):
            one(step_z, step_y)
        return carry

    lax.fori_loop(0, RING_Z - 1, plane, 0)
    for step_y in FAR_Y:
        one(0, step_y)
    pltpu.make_async_copy(source.at[mine], target.at[mine], receive).start()


def arrived(buffer, semaphore):
    pltpu.make_async_copy(buffer, buffer, semaphore).wait()


def spectral(
    cells_hbm, tables_hbm, conc_out, chem_out, total_out,
    cells, x_table, square, buffers, load_sems, send_sems, recv_sems, near_z, near_y, ring_y,
):
    row, col = lax.axis_index("row"), lax.axis_index("col")
    row_z, row_y = row // RING_Y, lax.rem(row, RING_Y)
    loads = [
        pltpu.make_async_copy(cells_hbm, cells, load_sems.at[0]),
        pltpu.make_async_copy(tables_hbm.at[pl.ds(0, 2)], x_table.at[0], load_sems.at[1]),
        pltpu.make_async_copy(tables_hbm.at[pl.ds(2, 2)], x_table.at[1], load_sems.at[2]),
        pltpu.make_async_copy(tables_hbm.at[pl.ds(4, 2)], square, load_sems.at[3]),
    ]
    barrier = pltpu.get_barrier_semaphore()
    at_z = [lax.rem(row_z + RING_Z + step, RING_Z) * RING_Y + row_y for step in NEAR_Z]
    at_y = [row_z * RING_Y + lax.rem(row_y + RING_Y + step, RING_Y) for step in NEAR_Y]
    around = [row_z * RING_Y + lax.rem(row_y + step, RING_Y) for step in FAR_Y]
    loads[0].start()
    for peer in at_z + at_y:
        signal(barrier, peer, col)
    for step in range(1, COLS):
        signal(barrier, row, lax.rem(col + step, COLS))
    for load in loads[1:]:
        load.start()

    lane = lax.broadcasted_iota(jnp.int32, (16, LANES), 1)
    first = lane < SLOTS
    loads[0].wait()
    conc = jnp.concatenate([cells[:, 0, :], jnp.zeros((16 - YB, NX), jnp.float32)])
    chem = conc * conc * conc - conc
    both = jnp.concatenate([conc, chem])
    folded = (both[:, :HALF] + both[:, HALF:], both[:, :HALF] - both[:, HALF:])
    out = buffers.at[0]
    for parity in range(2):
        loads[1 + parity].wait()
        spectrum = times_table(folded[parity], x_table.at[parity], ((1,), (0,)))
        for j in range(COLS // 2):
            part = spectrum[:, j * LANES:(j + 1) * LANES]
            top, bottom = part[:16], part[16:]
            base = (parity * (COLS // 2) + j) * BLOCK
            real = jnp.where(first, top, pltpu.roll(bottom, SLOTS, 1))
            imag = jnp.where(first, pltpu.roll(top, SLOTS, 1), bottom)
            out[base:base + YB, :] = real[:YB]
            out[base + YB:base + BLOCK, :] = imag[:YB]

    pl.semaphore_wait(barrier, len(at_z) + len(at_y) + COLS - 1)
    col_exchange(buffers.at[0], buffers.at[1], send_sems.at[0], recv_sems.at[0], row, col)
    for peer in at_z:
        signal(near_z, peer, col)
    for peer in at_y:
        signal(near_y, peer, col)
    loads[3].wait()


    def middle(k):
        rows, lanes = pl.ds(k // 2 * WIDE, WIDE), pl.ds(k % 2 * 256, WIDE)
        return square[0, rows, lanes], square[1, rows, lanes]

    lane_w = lax.broadcasted_iota(jnp.int32, (NZ, LANES), 1)
    kz = lax.broadcasted_iota(jnp.int32, (NZ, LANES), 0)
    slot = lax.rem(lane_w, SLOTS)
    low_col = col < COLS // 2
    kx = 2 * slot + jnp.where(low_col, 2 * EVEN * col, 2 * ODD * (col - COLS // 2) + 1)
    x_wave = kx.astype(jnp.float32) * (2.0 * math.pi / NX)
    y_wave = jnp.minimum(row, NY - row).astype(jnp.float32) * (2.0 * math.pi / NY)
    z_wave = jnp.minimum(kz, NZ - kz).astype(jnp.float32) * (2.0 * math.pi / NZ)
    squared = z_wave * z_wave + y_wave * y_wave + x_wave * x_wave
    damping = 1.0 / (1.0 + time_step * grad_coeff * squared * squared)
    mixing = jnp.where(lane_w < SLOTS, -time_step * squared, grad_coeff * squared)

    pl.semaphore_wait(near_z, len(at_z))
    pl.semaphore_wait(near_y, len(at_y))
    for peer in around:
        signal(ring_y, peer, col)
    arrived(buffers.at[1], recv_sems.at[0])
    buffers[2] = table_times(middle(0), buffers[1])
    pl.semaphore_wait(ring_y, len(around))
    row_exchange(buffers.at[2], buffers.at[3], send_sems.at[1], recv_sems.at[1], row, col)
    arrived(buffers.at[3], recv_sems.at[1])
    hat = table_times(middle(1), buffers[3])
    real, imag = hat[:NZ], hat[NZ:]
    real = (real + mixing * pltpu.roll(real, SLOTS, 1)) * damping
    imag = (imag + mixing * pltpu.roll(imag, SLOTS, 1)) * damping
    partial = jnp.sum(real * real + imag * imag, axis=0, keepdims=True)
    partial = jnp.broadcast_to(partial, (8, LANES))
    lane_8 = lax.broadcasted_iota(jnp.int32, (8, LANES), 1)
    sub_8 = lax.broadcasted_iota(jnp.int32, (8, LANES), 0)
    spare_8 = lax.rem(lane_8, SLOTS) >= EVEN
    chunks = [
        pltpu.roll(partial, (EVEN + SLOTS * (k % 2) - SPARE * k) % LANES, 1) for k in range(4)
    ]
    packed = jnp.where(
        lax.rem(sub_8, 2) == 0,
        jnp.where(lane_8 < SLOTS, chunks[0], chunks[1]),
        jnp.where(lane_8 < SLOTS, chunks[2], chunks[3]),
    )
    field = table_times(middle(2), jnp.concatenate([real, imag])).reshape(WIDE // 8, 8, LANES)
    buffers[4] = jnp.where(spare_8[None], packed[None], field).reshape(WIDE, LANES)
    row_exchange(buffers.at[4], buffers.at[5], send_sems.at[2], recv_sems.at[2], row, col)
    arrived(buffers.at[5], recv_sems.at[2])
    gathered = buffers[5]
    total = jnp.sum(gathered.reshape(WIDE // 8, 8, LANES), axis=0)
    total = total + pltpu.roll(total, 2, 0)
    total = total + pltpu.roll(total, 4, 0)
    even_total = jnp.broadcast_to(total[0:1], (BLOCK, LANES))
    odd_total = jnp.broadcast_to(total[1:2], (BLOCK, LANES))
    sub_b = lax.broadcasted_iota(jnp.int32, (BLOCK, LANES), 0)
    lane_b = lax.broadcasted_iota(jnp.int32, (BLOCK, LANES), 1)
    totals = jnp.where(sub_b < YB, even_total, odd_total)
    spare_b = lax.rem(lane_b, SLOTS) >= EVEN
    field = table_times(middle(3), gathered).reshape(COLS, BLOCK, LANES)
    buffers[6] = jnp.where(spare_b[None], totals[None], field).reshape(WIDE, LANES)
    col_exchange(buffers.at[6], buffers.at[7], send_sems.at[3], recv_sems.at[3], row, col)

    lane_1 = lax.broadcasted_iota(jnp.int32, (1, LANES), 1)
    slot_1 = lax.rem(lane_1, SLOTS)
    last = buffers.at[7]
    arrived(last, recv_sems.at[3])
    sums = []
    for parity in range(2):
        pieces = []
        for j in range(COLS // 2):
            c = parity * (COLS // 2) + j
            pad = jnp.zeros((16 - YB, LANES), jnp.float32)
            real = jnp.concatenate([last[c * BLOCK:c * BLOCK + YB, :], pad])
            imag = jnp.concatenate([last[c * BLOCK + YB:(c + 1) * BLOCK, :], pad])
            plane = plane_of(c, slot_1, jnp)
            keep = plane >= 0
            edge = (plane == 0) | (plane == NX // 2)
            scale = jnp.where(edge, 1.0, 2.0) / float(NX * NY * NZ)
            top = jnp.where(first, real, pltpu.roll(imag, SLOTS, 1))
            bottom = jnp.where(first, pltpu.roll(real, SLOTS, 1), imag)
            pieces.append(jnp.where(keep, jnp.concatenate([top, bottom]) * scale, 0.0))
        sums.append(times_table(jnp.concatenate(pieces, axis=1), x_table.at[parity], ((1,), (1,))))
    front, back = sums[0] + sums[1], sums[0] - sums[1]
    conc_out[:, 0, :HALF] = front[:YB]
    conc_out[:, 0, HALF:] = back[:YB]
    chem_out[:, 0, :HALF] = front[16:16 + YB]
    chem_out[:, 0, HALF:] = back[16:16 + YB]

    for c in range(COLS):
        for part in range(2):
            at = c * BLOCK + part * YB
            total_out[2 * c + part:2 * c + part + 1, :] = last[at:at + 1, :]

    for i, (buffer, left) in enumerate(((0, BLOCK), (2, 2), (4, 2), (6, BLOCK))):
        sent = buffers.at[buffer, pl.ds(0, WIDE - left)]
        arrived(sent, send_sems.at[i])


def hand_out(counts, conc, chem, total, conc_out, chem_out, power_out, power_held, sems):
    copies = [
        pltpu.make_async_copy(source, target, sems.at[i])
        for i, (source, target) in enumerate(((conc, conc_out), (chem, chem_out), (power_held, power_out)))
    ]
    copies[0].start()
    copies[1].start()
    col = lax.axis_index("col")
    lane_c = lax.broadcasted_iota(jnp.int32, (1, COLS), 1)
    owned = counts[...]
    start = jnp.sum(jnp.where(lane_c < col, owned, 0), axis=1, keepdims=True)
    mine = jnp.sum(jnp.where(lane_c == col, owned, 0), axis=1, keepdims=True)
    wanted = lax.broadcasted_iota(jnp.int32, (80, LANES), 0) + start
    lane_1 = lax.broadcasted_iota(jnp.int32, (1, LANES), 1)
    slot_1 = lax.rem(lane_1, SLOTS)
    found = jnp.zeros((80, LANES), jnp.float32)
    for c in range(COLS):
        for part in range(2):
            values = jnp.broadcast_to(total[2 * c + part:2 * c + part + 1, :], (80, LANES))
            packed = SPARE * (2 * part + lane_1 // SLOTS) + slot_1 - EVEN
            plane = jnp.where((slot_1 >= EVEN) & (packed < EVEN), plane_of(c, packed, jnp), -1)
            found = found + jnp.where(plane == wanted, values, 0.0)
    power = lax.dot_general(
        jnp.ones((8, LANES), jnp.float32), found, (((1,), (1,)), ((), ())),
        precision=lax.Precision.HIGHEST, preferred_element_type=jnp.float32,
    )
    power = jnp.log(power * (1.0 / float(NX * NY * NY * NZ * NZ)) + power_floor)
    power = jnp.where(lax.broadcasted_iota(jnp.int32, (8, 80), 1) < mine, power, 0.0)
    power_held[...] = power[0:1, :KX_MOST]
    copies[2].start()
    for copy in copies:
        copy.wait()


def shards(concentration, plane_counts):
    table = jnp.asarray(tables())
    vmem = pl.BlockSpec(memory_space=pltpu.VMEM)
    hbm = pl.BlockSpec(memory_space=pltpu.HBM)
    cells = concentration.reshape(YB, 1, NX)
    field = jax.ShapeDtypeStruct((YB, 1, NX), jnp.float32)
    held = pl.pallas_call(
        spectral,
        out_shape=(field, field, jax.ShapeDtypeStruct((2 * COLS, LANES), jnp.float32)),
        in_specs=[hbm, hbm],
        out_specs=(vmem, vmem, vmem),
        scratch_shapes=[
            pltpu.VMEM(cells.shape, jnp.float32),
            pltpu.VMEM((2, 2, HALF, X_SHARE), jnp.bfloat16),
            pltpu.VMEM((2, HALF, X_SHARE), jnp.bfloat16),
            pltpu.VMEM((8, WIDE, LANES), jnp.float32),
            pltpu.SemaphoreType.DMA((4,)),
            pltpu.SemaphoreType.DMA((4,)),
            pltpu.SemaphoreType.DMA((4,)),
            pltpu.SemaphoreType.REGULAR,
            pltpu.SemaphoreType.REGULAR,
            pltpu.SemaphoreType.REGULAR,
        ],
        compiler_params=pltpu.CompilerParams(
            collective_id=0, has_side_effects=True, vmem_limit_bytes=VMEM - ROOM
        ),
    )(cells, table)
    conc, chem, power = pl.pallas_call(
        hand_out,
        out_shape=(field, field, jax.ShapeDtypeStruct((1, KX_MOST), jnp.float32)),
        in_specs=[vmem, vmem, vmem, vmem],
        out_specs=(hbm, hbm, hbm),
        scratch_shapes=[pltpu.VMEM((1, KX_MOST), jnp.float32), pltpu.SemaphoreType.DMA((3,))],
        compiler_params=pltpu.CompilerParams(vmem_limit_bytes=4 * 1024 * 1024),
    )(plane_counts.reshape(1, COLS), *held)
    return conc.reshape(1, YB, NX), chem.reshape(1, YB, NX), power.reshape(KX_MOST)


def solution(mesh):
    return jax.shard_map(
        shards,
        mesh=mesh,
        in_specs=(P("row", "col", None), P()),
        out_specs=(P("row", "col", None), P("row", "col", None), P("col")),
        check_vma=False,
    )
```

```python
import functools
import math

import jax
import jax.numpy as jnp
import numpy as np
from jax import lax
from jax.experimental import pallas as pl
from jax.experimental.pallas import tpu as pltpu
from jax.sharding import PartitionSpec as P

MESH = pl.DeviceIdType.MESH
NX, NY, NZ = 768, 96, 96
HALF = NX // 2
COLS, ROWS = 8, 96
RING_Z, RING_Y = 12, 8
FAR_Y = (4, 3, 5, 2, 6, 1, 7)
START_Y = (0, 1, 2, 3, 7, 6, 5, 4)
FAR_COL = (4, 5, 3, 2, 6, 7, 1, 0)
NEAR_Z = (1, 2, 3, -1, -2, -3)
NEAR_Y = (1, 2, -1, -2)
YB = NY // COLS
LANES = 128
SLOTS = 64
EVEN, ODD = 49, 48
SPARE = 15
PLANES = NX // 2 + 1
KX_MOST = 73
BLOCK = 2 * YB
WIDE = 2 * NY
X_SHARE = COLS // 2 * LANES
VMEM = 67_043_328
ROOM = 10_600_000

time_step = 16.0
grad_coeff = 1.0
power_floor = 1e-6


def split(table):
    high = table.astype(np.float32).astype(jnp.bfloat16)
    low = (table - high.astype(np.float64)).astype(np.float32).astype(jnp.bfloat16)
    return np.stack([high, low])


def plane_of(col, slot, np=np):
    even = 2 * (EVEN * col + slot)
    odd = 2 * (ODD * (col - COLS // 2) + slot) + 1
    in_even = (slot < EVEN) & (even < PLANES)
    in_odd = slot < ODD
    low_col = col < COLS // 2
    return np.where(low_col, np.where(in_even, even, -1), np.where(in_odd, odd, -1))


@functools.cache
def tables():
    col = np.arange(COLS)[:, None]
    slot = np.arange(SLOTS)[None, :]
    plane = plane_of(col, slot)
    used = plane >= 0
    cells = np.arange(HALF)[:, None, None]
    phase = 2.0 * math.pi / NX * ((cells * np.maximum(plane, 0)[None]) % NX)
    x_table = np.stack([np.cos(phase) * used, -np.sin(phase) * used], axis=2)
    x_table = x_table.reshape(HALF, 2, COLS // 2 * LANES).transpose(1, 0, 2)

    index = np.arange(96)
    phase = 2.0 * math.pi / 96 * ((index[:, None] * index[None, :]) % 96)
    cosine, sine = np.cos(phase), np.sin(phase)
    full = np.stack([np.stack([cosine, sine], 1), np.stack([-sine, cosine], 1)])
    full = full.reshape(2, 96, 2, 96)
    by_block = full.reshape(2, 96, 2, COLS, YB)
    y_forward = by_block.transpose(1, 0, 3, 2, 4).reshape(WIDE, WIDE)
    z_forward = full.transpose(0, 1, 3, 2).reshape(WIDE, WIDE)
    square = np.zeros((2, HALF, X_SHARE), jnp.bfloat16)
    for k, table in enumerate((y_forward, z_forward, z_forward.T, y_forward.T)):
        square[k // 2, :, k % 2 * 256:k % 2 * 256 + WIDE] = split(table).reshape(HALF, WIDE)
    return np.concatenate([split(x_table[0]), split(x_table[1]), square])


def halves(value):
    high = value.astype(jnp.bfloat16)
    low = (value - high.astype(jnp.float32)).astype(jnp.bfloat16)
    return high, low


def product(a, b, contract):
    return lax.dot_general(a, b, (contract, ((), ())), preferred_element_type=jnp.float32)


def table_times(table, value):
    rows, lanes = table.shape[0] // 2, value.shape[1]
    parts = product(table, jnp.concatenate(halves(value), axis=1), ((1,), (0,)))
    return parts[:rows, :lanes] + (parts[:rows, lanes:] + parts[rows:, :lanes])


def times_table(value, table, contract):
    high, low = halves(value)
    rows = value.shape[0]
    parts = product(jnp.concatenate([high, low]), table[0], contract)
    return parts[:rows] + (parts[rows:] + product(high, table[1], contract))


def signal(semaphore, row, col):
    pl.semaphore_signal(semaphore, inc=1, device_id=(row, col), device_id_type=MESH)


def col_exchange(source, target, send, receive, row, col, peers):
    mine = pl.ds(pl.multiple_of(col * BLOCK, 8), BLOCK)
    for peer in peers:
        theirs = pl.ds(pl.multiple_of(peer * BLOCK, 8), BLOCK)

        @pl.when(peer != col)
        def _():
            pltpu.make_async_remote_copy(
                source.at[theirs], target.at[mine], send, receive, device_id=(row, peer), device_id_type=MESH
            ).start()

        @pl.when(peer == col)
        def _():
            pltpu.make_async_copy(source.at[mine], target.at[mine], receive).start()


def row_exchange(source, target, send, receive, row, col):
    mine = pl.ds(2 * row, 2)
    row_z, row_y = row // RING_Y, lax.rem(row, RING_Y)

    def one(step_z, step_y):
        peer = lax.rem(row_z + step_z, RING_Z) * RING_Y + lax.rem(row_y + step_y, RING_Y)
        pltpu.make_async_remote_copy(
            source.at[pl.ds(2 * peer, 2)], target.at[mine], send, receive, device_id=(peer, col), device_id_type=MESH
        ).start()

    def plane(i, carry):
        step_z = RING_Z // 2 + (1 - 2 * lax.rem(i, 2)) * ((i + 1) // 2)
        for step_y in FAR_Y + (0,):
            one(step_z, step_y)
        return carry

    lax.fori_loop(0, RING_Z - 1, plane, 0)
    for step_y in FAR_Y:
        one(0, step_y)
    pltpu.make_async_copy(source.at[mine], target.at[mine], receive).start()


def row_return(source, target, send, receive, row, col):
    mine = pl.ds(2 * row, 2)

    def plane(z, carry):
        for y in START_Y:
            peer = z * RING_Y + y

            @pl.when(peer != row)
            def _():
                pltpu.make_async_remote_copy(
                    source.at[pl.ds(2 * peer, 2)], target.at[mine], send, receive,
                    device_id=(peer, col), device_id_type=MESH,
                ).start()

        return carry

    lax.fori_loop(0, RING_Z, plane, 0)
    pltpu.make_async_copy(source.at[mine], target.at[mine], receive).start()


def arrived(buffer, semaphore):
    pltpu.make_async_copy(buffer, buffer, semaphore).wait()


def spectral(
    cells_hbm, tables_hbm, conc_out, chem_out, total_out,
    cells, x_table, square, buffers, load_sems, send_sems, recv_sems, near_z, near_y, ring_y,
):
    row, col = lax.axis_index("row"), lax.axis_index("col")
    row_z, row_y = row // RING_Y, lax.rem(row, RING_Y)
    loads = [
        pltpu.make_async_copy(cells_hbm, cells, load_sems.at[0]),
        pltpu.make_async_copy(tables_hbm.at[pl.ds(0, 2)], x_table.at[0], load_sems.at[1]),
        pltpu.make_async_copy(tables_hbm.at[pl.ds(2, 2)], x_table.at[1], load_sems.at[2]),
        pltpu.make_async_copy(tables_hbm.at[pl.ds(4, 2)], square, load_sems.at[3]),
    ]
    barrier = pltpu.get_barrier_semaphore()
    at_z = [lax.rem(row_z + RING_Z + step, RING_Z) * RING_Y + row_y for step in NEAR_Z]
    at_y = [row_z * RING_Y + lax.rem(row_y + RING_Y + step, RING_Y) for step in NEAR_Y]
    around = [row_z * RING_Y + lax.rem(row_y + step, RING_Y) for step in FAR_Y]
    for load in loads:
        load.start()
    for peer in at_z + at_y:
        signal(barrier, peer, col)
    for step in range(1, COLS):
        signal(barrier, row, lax.rem(col + step, COLS))

    lane = lax.broadcasted_iota(jnp.int32, (16, LANES), 1)
    first = lane < SLOTS
    loads[0].wait()
    conc = jnp.concatenate([cells[:, 0, :], jnp.zeros((16 - YB, NX), jnp.float32)])
    chem = conc * conc * conc - conc
    both = jnp.concatenate([conc, chem])
    folded = (both[:, :HALF] + both[:, HALF:], both[:, :HALF] - both[:, HALF:])
    out = buffers.at[0]
    for parity in range(2):
        loads[1 + parity].wait()
        spectrum = times_table(folded[parity], x_table.at[parity], ((1,), (0,)))
        for j in range(COLS // 2):
            part = spectrum[:, j * LANES:(j + 1) * LANES]
            top, bottom = part[:16], part[16:]
            base = (parity * (COLS // 2) + j) * BLOCK
            real = jnp.where(first, top, pltpu.roll(bottom, SLOTS, 1))
            imag = jnp.where(first, pltpu.roll(top, SLOTS, 1), bottom)
            out[base:base + YB, :] = real[:YB]
            out[base + YB:base + BLOCK, :] = imag[:YB]
        if parity == 0:
            pl.semaphore_wait(barrier, len(at_z) + len(at_y) + COLS - 1)
            for peer in at_z:
                signal(near_z, peer, col)
            for peer in at_y:
                signal(near_y, peer, col)
        half = COLS // 2
        peers = [parity * half + lax.rem(col + step, half) for step in (2, 1, 3, 0)]
        col_exchange(buffers.at[0], buffers.at[1], send_sems.at[0], recv_sems.at[0], row, col, peers)

    loads[3].wait()


    def middle(k):
        return square[k // 2, :, pl.ds(k % 2 * 256, WIDE)]

    lane_w = lax.broadcasted_iota(jnp.int32, (NZ, LANES), 1)
    kz = lax.broadcasted_iota(jnp.int32, (NZ, LANES), 0)
    slot = lax.rem(lane_w, SLOTS)
    low_col = col < COLS // 2
    kx = 2 * slot + jnp.where(low_col, 2 * EVEN * col, 2 * ODD * (col - COLS // 2) + 1)
    x_wave = kx.astype(jnp.float32) * (2.0 * math.pi / NX)
    y_wave = jnp.minimum(row, NY - row).astype(jnp.float32) * (2.0 * math.pi / NY)
    z_wave = jnp.minimum(kz, NZ - kz).astype(jnp.float32) * (2.0 * math.pi / NZ)
    squared = z_wave * z_wave + y_wave * y_wave + x_wave * x_wave
    damping = 1.0 / (1.0 + time_step * grad_coeff * squared * squared)
    mixing = jnp.where(lane_w < SLOTS, -time_step * squared, grad_coeff * squared)

    pl.semaphore_wait(near_z, len(at_z))
    pl.semaphore_wait(near_y, len(at_y))
    for peer in around:
        signal(ring_y, peer, col)
    arrived(buffers.at[1], recv_sems.at[0])
    buffers[2] = table_times(middle(0), buffers[1])
    pl.semaphore_wait(ring_y, len(around))
    row_exchange(buffers.at[2], buffers.at[3], send_sems.at[1], recv_sems.at[1], row, col)
    arrived(buffers.at[3], recv_sems.at[1])
    hat = table_times(middle(1), buffers[3])
    real, imag = hat[:NZ], hat[NZ:]
    real = (real + mixing * pltpu.roll(real, SLOTS, 1)) * damping
    imag = (imag + mixing * pltpu.roll(imag, SLOTS, 1)) * damping
    partial = jnp.sum(real * real + imag * imag, axis=0, keepdims=True)
    partial = jnp.broadcast_to(partial, (8, LANES))
    lane_8 = lax.broadcasted_iota(jnp.int32, (8, LANES), 1)
    sub_8 = lax.broadcasted_iota(jnp.int32, (8, LANES), 0)
    spare_8 = lax.rem(lane_8, SLOTS) >= EVEN
    chunks = [
        pltpu.roll(partial, (EVEN + SLOTS * (k % 2) - SPARE * k) % LANES, 1) for k in range(4)
    ]
    packed = jnp.where(
        lax.rem(sub_8, 2) == 0,
        jnp.where(lane_8 < SLOTS, chunks[0], chunks[1]),
        jnp.where(lane_8 < SLOTS, chunks[2], chunks[3]),
    )
    field = table_times(middle(2), jnp.concatenate([real, imag])).reshape(WIDE // 8, 8, LANES)
    buffers[4] = jnp.where(spare_8[None], packed[None], field).reshape(WIDE, LANES)
    row_return(buffers.at[4], buffers.at[5], send_sems.at[2], recv_sems.at[2], row, col)
    arrived(buffers.at[5], recv_sems.at[2])
    gathered = buffers[5]
    total = jnp.sum(gathered.reshape(WIDE // 8, 8, LANES), axis=0)
    total = total + pltpu.roll(total, 2, 0)
    total = total + pltpu.roll(total, 4, 0)
    even_total = jnp.broadcast_to(total[0:1], (BLOCK, LANES))
    odd_total = jnp.broadcast_to(total[1:2], (BLOCK, LANES))
    sub_b = lax.broadcasted_iota(jnp.int32, (BLOCK, LANES), 0)
    lane_b = lax.broadcasted_iota(jnp.int32, (BLOCK, LANES), 1)
    totals = jnp.where(sub_b < YB, even_total, odd_total)
    spare_b = lax.rem(lane_b, SLOTS) >= EVEN
    field = table_times(middle(3), gathered).reshape(COLS, BLOCK, LANES)
    buffers[6] = jnp.where(spare_b[None], totals[None], field).reshape(WIDE, LANES)
    col_exchange(buffers.at[6], buffers.at[7], send_sems.at[3], recv_sems.at[3], row, col,
        [lax.rem(col + step, COLS) for step in FAR_COL])

    lane_1 = lax.broadcasted_iota(jnp.int32, (1, LANES), 1)
    slot_1 = lax.rem(lane_1, SLOTS)
    last = buffers.at[7]
    arrived(last, recv_sems.at[3])
    sums = []
    for parity in range(2):
        pieces = []
        for j in range(COLS // 2):
            c = parity * (COLS // 2) + j
            pad = jnp.zeros((16 - YB, LANES), jnp.float32)
            real = jnp.concatenate([last[c * BLOCK:c * BLOCK + YB, :], pad])
            imag = jnp.concatenate([last[c * BLOCK + YB:(c + 1) * BLOCK, :], pad])
            plane = plane_of(c, slot_1, jnp)
            keep = plane >= 0
            edge = (plane == 0) | (plane == NX // 2)
            scale = jnp.where(edge, 1.0, 2.0) / float(NX * NY * NZ)
            top = jnp.where(first, real, pltpu.roll(imag, SLOTS, 1))
            bottom = jnp.where(first, pltpu.roll(real, SLOTS, 1), imag)
            pieces.append(jnp.where(keep, jnp.concatenate([top, bottom]) * scale, 0.0))
        sums.append(times_table(jnp.concatenate(pieces, axis=1), x_table.at[parity], ((1,), (1,))))
    front, back = sums[0] + sums[1], sums[0] - sums[1]
    conc_out[:, 0, :HALF] = front[:YB]
    conc_out[:, 0, HALF:] = back[:YB]
    chem_out[:, 0, :HALF] = front[16:16 + YB]
    chem_out[:, 0, HALF:] = back[16:16 + YB]

    for c in range(COLS):
        for part in range(2):
            at = c * BLOCK + part * YB
            total_out[2 * c + part:2 * c + part + 1, :] = last[at:at + 1, :]

    for i, (buffer, left) in enumerate(((0, BLOCK), (2, 2), (4, 2), (6, BLOCK))):
        sent = buffers.at[buffer, pl.ds(0, WIDE - left)]
        arrived(sent, send_sems.at[i])


def hand_out(counts, conc, chem, total, conc_out, chem_out, power_out, power_held, sems):
    copies = [
        pltpu.make_async_copy(source, target, sems.at[i])
        for i, (source, target) in enumerate(((conc, conc_out), (chem, chem_out), (power_held, power_out)))
    ]
    copies[0].start()
    copies[1].start()
    col = lax.axis_index("col")
    lane_c = lax.broadcasted_iota(jnp.int32, (1, COLS), 1)
    owned = counts[...]
    start = jnp.sum(jnp.where(lane_c < col, owned, 0), axis=1, keepdims=True)
    mine = jnp.sum(jnp.where(lane_c == col, owned, 0), axis=1, keepdims=True)
    wanted = lax.broadcasted_iota(jnp.int32, (80, LANES), 0) + start
    lane_1 = lax.broadcasted_iota(jnp.int32, (1, LANES), 1)
    slot_1 = lax.rem(lane_1, SLOTS)
    found = jnp.zeros((80, LANES), jnp.float32)
    for c in range(COLS):
        for part in range(2):
            values = jnp.broadcast_to(total[2 * c + part:2 * c + part + 1, :], (80, LANES))
            packed = SPARE * (2 * part + lane_1 // SLOTS) + slot_1 - EVEN
            plane = jnp.where((slot_1 >= EVEN) & (packed < EVEN), plane_of(c, packed, jnp), -1)
            found = found + jnp.where(plane == wanted, values, 0.0)
    power = lax.dot_general(
        jnp.ones((8, LANES), jnp.float32), found, (((1,), (1,)), ((), ())),
        precision=lax.Precision.HIGHEST, preferred_element_type=jnp.float32,
    )
    power = jnp.log(power * (1.0 / float(NX * NY * NY * NZ * NZ)) + power_floor)
    power = jnp.where(lax.broadcasted_iota(jnp.int32, (8, 80), 1) < mine, power, 0.0)
    power_held[...] = power[0:1, :KX_MOST]
    copies[2].start()
    for copy in copies:
        copy.wait()


def shards(concentration, plane_counts):
    table = jnp.asarray(tables())
    vmem = pl.BlockSpec(memory_space=pltpu.VMEM)
    hbm = pl.BlockSpec(memory_space=pltpu.HBM)
    cells = concentration.reshape(YB, 1, NX)
    field = jax.ShapeDtypeStruct((YB, 1, NX), jnp.float32)
    held = pl.pallas_call(
        spectral,
        out_shape=(field, field, jax.ShapeDtypeStruct((2 * COLS, LANES), jnp.float32)),
        in_specs=[hbm, hbm],
        out_specs=(vmem, vmem, vmem),
        scratch_shapes=[
            pltpu.VMEM(cells.shape, jnp.float32),
            pltpu.VMEM((2, 2, HALF, X_SHARE), jnp.bfloat16),
            pltpu.VMEM((2, HALF, X_SHARE), jnp.bfloat16),
            pltpu.VMEM((8, WIDE, LANES), jnp.float32),
            pltpu.SemaphoreType.DMA((4,)),
            pltpu.SemaphoreType.DMA((4,)),
            pltpu.SemaphoreType.DMA((4,)),
            pltpu.SemaphoreType.REGULAR,
            pltpu.SemaphoreType.REGULAR,
            pltpu.SemaphoreType.REGULAR,
        ],
        compiler_params=pltpu.CompilerParams(
            collective_id=0, has_side_effects=True, vmem_limit_bytes=VMEM - ROOM
        ),
    )(cells, table)
    conc, chem, power = pl.pallas_call(
        hand_out,
        out_shape=(field, field, jax.ShapeDtypeStruct((1, KX_MOST), jnp.float32)),
        in_specs=[vmem, vmem, vmem, vmem],
        out_specs=(hbm, hbm, hbm),
        scratch_shapes=[pltpu.VMEM((1, KX_MOST), jnp.float32), pltpu.SemaphoreType.DMA((3,))],
        compiler_params=pltpu.CompilerParams(vmem_limit_bytes=4 * 1024 * 1024),
    )(plane_counts.reshape(1, COLS), *held)
    return conc.reshape(1, YB, NX), chem.reshape(1, YB, NX), power.reshape(KX_MOST)


def solution(mesh):
    return jax.shard_map(
        shards,
        mesh=mesh,
        in_specs=(P("row", "col", None), P()),
        out_specs=(P("row", "col", None), P("row", "col", None), P("col")),
        check_vma=False,
    )
```

```python
import functools
import math

import jax
import jax.numpy as jnp
import numpy as np
from jax import lax
from jax.experimental import pallas as pl
from jax.experimental.pallas import tpu as pltpu
from jax.sharding import PartitionSpec as P

MESH = pl.DeviceIdType.MESH
NX, NY, NZ = 768, 96, 96
HALF = NX // 2
COLS, ROWS = 8, 96
RING_Z, RING_Y = 12, 8
FAR_Y = (4, 3, 5, 2, 6, 1, 7)
FAR_Z = (6, 5, 7, 4, 8, 3, 9, 2, 10, 1, 11)
START_Y = (0, 1, 2, 3, 7, 6, 5, 4)
FAR_COL = (4, 5, 3, 2, 6, 7, 1, 0)
NEAR_Z = (1, 2, 3, -1, -2, -3)
NEAR_Y = (1, 2, -1, -2)
YB = NY // COLS
LANES = 128
SLOTS = 64
EVEN, ODD = 49, 48
SPARE = 15
PLANES = NX // 2 + 1
KX_MOST = 73
BLOCK = 2 * YB
WIDE = 2 * NY
X_SHARE = COLS // 2 * LANES
VMEM = 67_043_328
ROOM = 10_600_000

time_step = 16.0
grad_coeff = 1.0
power_floor = 1e-6


def split(table):
    high = table.astype(np.float32).astype(jnp.bfloat16)
    low = (table - high.astype(np.float64)).astype(np.float32).astype(jnp.bfloat16)
    return np.stack([high, low])


def plane_of(col, slot, np=np):
    even = 2 * (EVEN * col + slot)
    odd = 2 * (ODD * (col - COLS // 2) + slot) + 1
    in_even = (slot < EVEN) & (even < PLANES)
    in_odd = slot < ODD
    low_col = col < COLS // 2
    return np.where(low_col, np.where(in_even, even, -1), np.where(in_odd, odd, -1))


@functools.cache
def tables():
    col = np.arange(COLS)[:, None]
    slot = np.arange(SLOTS)[None, :]
    plane = plane_of(col, slot)
    used = plane >= 0
    cells = np.arange(HALF)[:, None, None]
    phase = 2.0 * math.pi / NX * ((cells * np.maximum(plane, 0)[None]) % NX)
    x_table = np.stack([np.cos(phase) * used, -np.sin(phase) * used], axis=2)
    x_table = x_table.reshape(HALF, 2, COLS // 2 * LANES).transpose(1, 0, 2)

    index = np.arange(96)
    phase = 2.0 * math.pi / 96 * ((index[:, None] * index[None, :]) % 96)
    cosine, sine = np.cos(phase), np.sin(phase)
    full = np.stack([np.stack([cosine, sine], 1), np.stack([-sine, cosine], 1)])
    full = full.reshape(2, 96, 2, 96)
    by_block = full.reshape(2, 96, 2, COLS, YB)
    y_forward = by_block.transpose(1, 0, 3, 2, 4).reshape(WIDE, WIDE)
    z_forward = full.transpose(0, 1, 3, 2).reshape(WIDE, WIDE)
    square = np.zeros((2, HALF, X_SHARE), jnp.bfloat16)
    for k, table in enumerate((y_forward, z_forward, z_forward.T, y_forward.T)):
        square[k // 2, :, k % 2 * 256:k % 2 * 256 + WIDE] = split(table).reshape(HALF, WIDE)
    return np.concatenate([split(x_table[0]), split(x_table[1]), square])


def halves(value):
    high = value.astype(jnp.bfloat16)
    low = (value - high.astype(jnp.float32)).astype(jnp.bfloat16)
    return high, low


def product(a, b, contract):
    return lax.dot_general(a, b, (contract, ((), ())), preferred_element_type=jnp.float32)


def table_times(table, value):
    rows, lanes = table.shape[0] // 2, value.shape[1]
    parts = product(table, jnp.concatenate(halves(value), axis=1), ((1,), (0,)))
    return parts[:rows, :lanes] + (parts[:rows, lanes:] + parts[rows:, :lanes])


def times_table(value, table, contract):
    high, low = halves(value)
    rows = value.shape[0]
    parts = product(jnp.concatenate([high, low]), table[0], contract)
    return parts[:rows] + (parts[rows:] + product(high, table[1], contract))


def signal(semaphore, row, col):
    pl.semaphore_signal(semaphore, inc=1, device_id=(row, col), device_id_type=MESH)


def col_exchange(source, target, send, receive, row, col, peers):
    mine = pl.ds(pl.multiple_of(col * BLOCK, 8), BLOCK)
    for peer in peers:
        theirs = pl.ds(pl.multiple_of(peer * BLOCK, 8), BLOCK)

        @pl.when(peer != col)
        def _():
            pltpu.make_async_remote_copy(
                source.at[theirs], target.at[mine], send, receive, device_id=(row, peer), device_id_type=MESH
            ).start()

        @pl.when(peer == col)
        def _():
            pltpu.make_async_copy(source.at[mine], target.at[mine], receive).start()


def row_exchange(source, target, send, receive, row, col, ring_y):
    mine = pl.ds(2 * row, 2)
    row_z, row_y = row // RING_Y, lax.rem(row, RING_Y)
    far_z = [lax.rem(row_z + step, RING_Z) * RING_Y for step in FAR_Z]

    def one(peer):
        pltpu.make_async_remote_copy(
            source.at[pl.ds(2 * peer, 2)], target.at[mine], send, receive, device_id=(peer, col), device_id_type=MESH
        ).start()

    def column(i, carry):
        y = i + i // 4 * (11 - 2 * i)

        @pl.when(y != row_y)
        def _():
            pl.semaphore_wait(ring_y.at[y], 1)
            for first in far_z:
                one(first + y)
            one(row_z * RING_Y + y)

        return carry

    for first in far_z:
        one(first + row_y)
    pltpu.make_async_copy(source.at[mine], target.at[mine], receive).start()
    lax.fori_loop(0, RING_Y, column, 0)


def row_return(source, target, send, receive, row, col):
    mine = pl.ds(2 * row, 2)

    def plane(z, carry):
        for y in START_Y:
            peer = z * RING_Y + y

            @pl.when(peer != row)
            def _():
                pltpu.make_async_remote_copy(
                    source.at[pl.ds(2 * peer, 2)], target.at[mine], send, receive,
                    device_id=(peer, col), device_id_type=MESH,
                ).start()

        return carry

    lax.fori_loop(0, RING_Z, plane, 0)
    pltpu.make_async_copy(source.at[mine], target.at[mine], receive).start()


def arrived(buffer, semaphore):
    pltpu.make_async_copy(buffer, buffer, semaphore).wait()


def spectral(
    cells_hbm, tables_hbm, conc_out, chem_out, total_out,
    cells, x_table, square, buffers, load_sems, send_sems, recv_sems, near_z, near_y, ring_y,
):
    row, col = lax.axis_index("row"), lax.axis_index("col")
    row_z, row_y = row // RING_Y, lax.rem(row, RING_Y)
    loads = [
        pltpu.make_async_copy(cells_hbm, cells, load_sems.at[0]),
        pltpu.make_async_copy(tables_hbm.at[pl.ds(0, 2)], x_table.at[0], load_sems.at[1]),
        pltpu.make_async_copy(tables_hbm.at[pl.ds(2, 2)], x_table.at[1], load_sems.at[2]),
        pltpu.make_async_copy(tables_hbm.at[pl.ds(4, 2)], square, load_sems.at[3]),
    ]
    barrier = pltpu.get_barrier_semaphore()
    at_z = [lax.rem(row_z + RING_Z + step, RING_Z) * RING_Y + row_y for step in NEAR_Z]
    at_y = [row_z * RING_Y + lax.rem(row_y + RING_Y + step, RING_Y) for step in NEAR_Y]
    around = [row_z * RING_Y + lax.rem(row_y + step, RING_Y) for step in FAR_Y]
    for peer in at_z + at_y:
        signal(barrier, peer, col)
    for step in range(1, COLS):
        signal(barrier, row, lax.rem(col + step, COLS))
    for load in loads:
        load.start()

    pl.semaphore_wait(barrier, len(at_z) + len(at_y) + COLS - 1)
    for peer in at_z:
        signal(near_z, peer, col)
    for peer in at_y:
        signal(near_y, peer, col)

    lane = lax.broadcasted_iota(jnp.int32, (16, LANES), 1)
    first = lane < SLOTS
    loads[0].wait()
    conc = jnp.concatenate([cells[:, 0, :], jnp.zeros((16 - YB, NX), jnp.float32)])
    chem = conc * conc * conc - conc
    both = jnp.concatenate([conc, chem])
    folded = (both[:, :HALF] + both[:, HALF:], both[:, :HALF] - both[:, HALF:])
    out = buffers.at[0]
    for parity in range(2):
        loads[1 + parity].wait()
        spectrum = times_table(folded[parity], x_table.at[parity], ((1,), (0,)))
        for j in range(COLS // 2):
            part = spectrum[:, j * LANES:(j + 1) * LANES]
            top, bottom = part[:16], part[16:]
            base = (parity * (COLS // 2) + j) * BLOCK
            real = jnp.where(first, top, pltpu.roll(bottom, SLOTS, 1))
            imag = jnp.where(first, pltpu.roll(top, SLOTS, 1), bottom)
            out[base:base + YB, :] = real[:YB]
            out[base + YB:base + BLOCK, :] = imag[:YB]
        half = COLS // 2
        peers = [parity * half + lax.rem(col + step, half) for step in (2, 1, 3, 0)]
        col_exchange(buffers.at[0], buffers.at[1], send_sems.at[0], recv_sems.at[0], row, col, peers)

    pl.semaphore_wait(near_z, len(at_z))
    pl.semaphore_wait(near_y, len(at_y))
    for peer in around:
        signal(ring_y.at[row_y], peer, col)
    loads[3].wait()


    def middle(k):
        return square[k // 2, :, pl.ds(k % 2 * 256, WIDE)]

    lane_w = lax.broadcasted_iota(jnp.int32, (NZ, LANES), 1)
    kz = lax.broadcasted_iota(jnp.int32, (NZ, LANES), 0)
    slot = lax.rem(lane_w, SLOTS)
    low_col = col < COLS // 2
    kx = 2 * slot + jnp.where(low_col, 2 * EVEN * col, 2 * ODD * (col - COLS // 2) + 1)
    x_wave = kx.astype(jnp.float32) * (2.0 * math.pi / NX)
    y_wave = jnp.minimum(row, NY - row).astype(jnp.float32) * (2.0 * math.pi / NY)
    z_wave = jnp.minimum(kz, NZ - kz).astype(jnp.float32) * (2.0 * math.pi / NZ)
    squared = z_wave * z_wave + y_wave * y_wave + x_wave * x_wave
    damping = 1.0 / (1.0 + time_step * grad_coeff * squared * squared)
    mixing = jnp.where(lane_w < SLOTS, -time_step * squared, grad_coeff * squared)

    arrived(buffers.at[1], recv_sems.at[0])
    buffers[2] = table_times(middle(0), buffers[1])
    row_exchange(buffers.at[2], buffers.at[3], send_sems.at[1], recv_sems.at[1], row, col, ring_y)
    arrived(buffers.at[3], recv_sems.at[1])
    hat = table_times(middle(1), buffers[3])
    real, imag = hat[:NZ], hat[NZ:]
    real = (real + mixing * pltpu.roll(real, SLOTS, 1)) * damping
    imag = (imag + mixing * pltpu.roll(imag, SLOTS, 1)) * damping
    partial = jnp.sum(real * real + imag * imag, axis=0, keepdims=True)
    partial = jnp.broadcast_to(partial, (8, LANES))
    lane_8 = lax.broadcasted_iota(jnp.int32, (8, LANES), 1)
    sub_8 = lax.broadcasted_iota(jnp.int32, (8, LANES), 0)
    spare_8 = lax.rem(lane_8, SLOTS) >= EVEN
    chunks = [
        pltpu.roll(partial, (EVEN + SLOTS * (k % 2) - SPARE * k) % LANES, 1) for k in range(4)
    ]
    packed = jnp.where(
        lax.rem(sub_8, 2) == 0,
        jnp.where(lane_8 < SLOTS, chunks[0], chunks[1]),
        jnp.where(lane_8 < SLOTS, chunks[2], chunks[3]),
    )
    field = table_times(middle(2), jnp.concatenate([real, imag])).reshape(WIDE // 8, 8, LANES)
    buffers[4] = jnp.where(spare_8[None], packed[None], field).reshape(WIDE, LANES)
    row_return(buffers.at[4], buffers.at[5], send_sems.at[2], recv_sems.at[2], row, col)
    arrived(buffers.at[5], recv_sems.at[2])
    gathered = buffers[5]
    total = jnp.sum(gathered.reshape(WIDE // 8, 8, LANES), axis=0)
    total = total + pltpu.roll(total, 2, 0)
    total = total + pltpu.roll(total, 4, 0)
    even_total = jnp.broadcast_to(total[0:1], (BLOCK, LANES))
    odd_total = jnp.broadcast_to(total[1:2], (BLOCK, LANES))
    sub_b = lax.broadcasted_iota(jnp.int32, (BLOCK, LANES), 0)
    lane_b = lax.broadcasted_iota(jnp.int32, (BLOCK, LANES), 1)
    totals = jnp.where(sub_b < YB, even_total, odd_total)
    spare_b = lax.rem(lane_b, SLOTS) >= EVEN
    field = table_times(middle(3), gathered).reshape(COLS, BLOCK, LANES)
    buffers[6] = jnp.where(spare_b[None], totals[None], field).reshape(WIDE, LANES)
    col_exchange(buffers.at[6], buffers.at[7], send_sems.at[3], recv_sems.at[3 + col // (COLS // 2)], row, col,
        [lax.rem(col + step, COLS) for step in FAR_COL])

    lane_1 = lax.broadcasted_iota(jnp.int32, (1, LANES), 1)
    slot_1 = lax.rem(lane_1, SLOTS)
    last = buffers.at[7]
    sums = []
    for parity in range(2):
        arrived(buffers.at[7, pl.ds(parity * (WIDE // 2), WIDE // 2)], recv_sems.at[3 + parity])
        pieces = []
        for j in range(COLS // 2):
            c = parity * (COLS // 2) + j
            pad = jnp.zeros((16 - YB, LANES), jnp.float32)
            real = jnp.concatenate([last[c * BLOCK:c * BLOCK + YB, :], pad])
            imag = jnp.concatenate([last[c * BLOCK + YB:(c + 1) * BLOCK, :], pad])
            plane = plane_of(c, slot_1, jnp)
            keep = plane >= 0
            edge = (plane == 0) | (plane == NX // 2)
            scale = jnp.where(edge, 1.0, 2.0) / float(NX * NY * NZ)
            top = jnp.where(first, real, pltpu.roll(imag, SLOTS, 1))
            bottom = jnp.where(first, pltpu.roll(real, SLOTS, 1), imag)
            pieces.append(jnp.where(keep, jnp.concatenate([top, bottom]) * scale, 0.0))
        sums.append(times_table(jnp.concatenate(pieces, axis=1), x_table.at[parity], ((1,), (1,))))
    front, back = sums[0] + sums[1], sums[0] - sums[1]
    conc_out[:, 0, :HALF] = front[:YB]
    conc_out[:, 0, HALF:] = back[:YB]
    chem_out[:, 0, :HALF] = front[16:16 + YB]
    chem_out[:, 0, HALF:] = back[16:16 + YB]

    for c in range(COLS):
        for part in range(2):
            at = c * BLOCK + part * YB
            total_out[2 * c + part:2 * c + part + 1, :] = last[at:at + 1, :]

    for i, (buffer, left) in enumerate(((0, BLOCK), (2, 2), (4, 2), (6, BLOCK))):
        sent = buffers.at[buffer, pl.ds(0, WIDE - left)]
        arrived(sent, send_sems.at[i])


def hand_out(counts, conc, chem, total, conc_out, chem_out, power_out, power_held, sems):
    copies = [
        pltpu.make_async_copy(source, target, sems.at[i])
        for i, (source, target) in enumerate(((conc, conc_out), (chem, chem_out), (power_held, power_out)))
    ]
    copies[0].start()
    copies[1].start()
    col = lax.axis_index("col")
    lane_c = lax.broadcasted_iota(jnp.int32, (1, COLS), 1)
    owned = counts[...]
    start = jnp.sum(jnp.where(lane_c < col, owned, 0), axis=1, keepdims=True)
    mine = jnp.sum(jnp.where(lane_c == col, owned, 0), axis=1, keepdims=True)
    wanted = lax.broadcasted_iota(jnp.int32, (80, LANES), 0) + start
    lane_1 = lax.broadcasted_iota(jnp.int32, (1, LANES), 1)
    slot_1 = lax.rem(lane_1, SLOTS)
    found = jnp.zeros((80, LANES), jnp.float32)
    for c in range(COLS):
        for part in range(2):
            values = jnp.broadcast_to(total[2 * c + part:2 * c + part + 1, :], (80, LANES))
            packed = SPARE * (2 * part + lane_1 // SLOTS) + slot_1 - EVEN
            plane = jnp.where((slot_1 >= EVEN) & (packed < EVEN), plane_of(c, packed, jnp), -1)
            found = found + jnp.where(plane == wanted, values, 0.0)
    power = lax.dot_general(
        jnp.ones((8, LANES), jnp.float32), found, (((1,), (1,)), ((), ())),
        precision=lax.Precision.HIGHEST, preferred_element_type=jnp.float32,
    )
    power = jnp.log(power * (1.0 / float(NX * NY * NY * NZ * NZ)) + power_floor)
    power = jnp.where(lax.broadcasted_iota(jnp.int32, (8, 80), 1) < mine, power, 0.0)
    power_held[...] = power[0:1, :KX_MOST]
    copies[2].start()
    for copy in copies:
        copy.wait()


def shards(concentration, plane_counts):
    table = jnp.asarray(tables())
    vmem = pl.BlockSpec(memory_space=pltpu.VMEM)
    hbm = pl.BlockSpec(memory_space=pltpu.HBM)
    cells = concentration.reshape(YB, 1, NX)
    field = jax.ShapeDtypeStruct((YB, 1, NX), jnp.float32)
    held = pl.pallas_call(
        spectral,
        out_shape=(field, field, jax.ShapeDtypeStruct((2 * COLS, LANES), jnp.float32)),
        in_specs=[hbm, hbm],
        out_specs=(vmem, vmem, vmem),
        scratch_shapes=[
            pltpu.VMEM(cells.shape, jnp.float32),
            pltpu.VMEM((2, 2, HALF, X_SHARE), jnp.bfloat16),
            pltpu.VMEM((2, HALF, X_SHARE), jnp.bfloat16),
            pltpu.VMEM((8, WIDE, LANES), jnp.float32),
            pltpu.SemaphoreType.DMA((4,)),
            pltpu.SemaphoreType.DMA((4,)),
            pltpu.SemaphoreType.DMA((5,)),
            pltpu.SemaphoreType.REGULAR,
            pltpu.SemaphoreType.REGULAR,
            pltpu.SemaphoreType.REGULAR((RING_Y,)),
        ],
        compiler_params=pltpu.CompilerParams(
            collective_id=0, has_side_effects=True, vmem_limit_bytes=VMEM - ROOM
        ),
    )(cells, table)
    conc, chem, power = pl.pallas_call(
        hand_out,
        out_shape=(field, field, jax.ShapeDtypeStruct((1, KX_MOST), jnp.float32)),
        in_specs=[vmem, vmem, vmem, vmem],
        out_specs=(hbm, hbm, hbm),
        scratch_shapes=[pltpu.VMEM((1, KX_MOST), jnp.float32), pltpu.SemaphoreType.DMA((3,))],
        compiler_params=pltpu.CompilerParams(vmem_limit_bytes=4 * 1024 * 1024),
    )(plane_counts.reshape(1, COLS), *held)
    return conc.reshape(1, YB, NX), chem.reshape(1, YB, NX), power.reshape(KX_MOST)


def solution(mesh):
    return jax.shard_map(
        shards,
        mesh=mesh,
        in_specs=(P("row", "col", None), P()),
        out_specs=(P("row", "col", None), P("row", "col", None), P("col")),
        check_vma=False,
    )
```
